32 devices in a mesh: pairs: 2 (over x), ctx: 16 (over z, y, core).
Axes of the slice: x: 2, y: 2, z: 4, core: 2. Of those that a mesh axis runs over, the one named last changes fastest.
Arguments:
- prompt_keys: bfloat16 [1024, 512], P(('pairs', 'ctx')), parts along dimension 0, may hold values from -4 to 4
- prompt_values: bfloat16 [1024, 512], P(('pairs', 'ctx')), parts along dimension 0, may hold values from -6 to 6
- queries: bfloat16 [4, 768, 4096], P('pairs', 'ctx'), parts along dimension 0, may hold values from -100 to 100
- resp_keys: bfloat16 [4, 768, 512], P('pairs', 'ctx'), parts along dimension 0, may hold values from -6 to 6
- resp_values: bfloat16 [4, 768, 512], P('pairs', 'ctx'), parts along dimension 0, may hold values from -6 to 6
- cotangent: bfloat16 [4, 768, 4096], P('pairs', 'ctx'), parts along dimension 0, may hold values from -48 to 48
- lengths: int32 [4], P('pairs'), parts along dimension 0, may hold values from 192 to 768, as said below
Outputs:
- grad_queries: float32 [4, 768, 4096], P('pairs', 'ctx'), parts along dimension 0
- grad_resp_keys: float32 [4, 768, 512], P('pairs', 'ctx'), parts along dimension 0
- grad_resp_values: float32 [4, 768, 512], P('pairs', 'ctx'), parts along dimension 0
- grad_prompt_keys: float32 [1024, 512], P(('pairs', 'ctx')), parts along dimension 0
- grad_prompt_values: float32 [1024, 512], P(('pairs', 'ctx')), parts along dimension 0
The draws below stay inside these ranges and needn't reach their ends.
There are 2 independent parts, one for each index of `pairs`. The reference program is written for one: setup_inputs(seed, part) draws one part's arguments, and reference() takes and returns one part's arrays. A program takes and returns all parts, laid end to end along the dimension named above; each array names one. Nothing has to cross between parts.
Inputs may be any that keep to these rules, and one draw needn't show every extreme that they name: `lengths`: in every pair one of the two responses has all 768 rows live.
All inputs are finite; a program needn't handle non-finite values.
Results may differ from the reference program's by a relative error of at most 0.005.
Values may be sent and summed in bfloat16 or wider, within the bound.
A program may use at most 128 MiB of HBM per device.

```python
import math
import jax
import jax.numpy as jnp
from jax import lax

HEADS = 32
KV_HEADS = 4
HEAD_DIM = 128
RESP = 768
PROMPT = 512


def prompt_draw(key):
    return jax.random.truncated_normal(jax.random.fold_in(key, 11), -4.0, 4.0, (PROMPT, KV_HEADS * HEAD_DIM), jnp.float32)


def draw_prompt_keys(key, part):
    return prompt_draw(key).astype(jnp.bfloat16)


def draw_queries(key, part):
    normal_part = jax.random.normal(jax.random.fold_in(key, 23), (2, RESP, HEADS * HEAD_DIM), jnp.float32)
    result = jnp.clip(normal_part, -6.0, 6.0)
    return result.astype(jnp.bfloat16)


def draw_lengths(key, part):
    shorter = jax.random.randint(jax.random.fold_in(key, 41), (), RESP // 4, RESP + 1).astype(jnp.int32)
    longer = jnp.full((), RESP, jnp.int32)
    which = jax.random.randint(jax.random.fold_in(key, 43), (), 0, 2)
    return jnp.where(which == 0, jnp.stack([longer, shorter]), jnp.stack([shorter, longer])).astype(jnp.int32)


def level_of(key, dims, pieces, least, high):
    level, own = 1.0, jax.random.fold_in(key, 6)
    for position, shards_of in pieces:
        draws = jnp.exp(jax.random.uniform(jax.random.fold_in(own, position), (shards_of,), jnp.float32, least / len(pieces), high / len(pieces)))
        level = level * jnp.repeat(draws, dims[position] // shards_of).reshape([-1 if axis == position else 1 for axis in range(len(dims))])
    return level


def bell_draw(own_key, shape, deviation, limit, cuts=(), kind=jnp.bfloat16):
    values = jax.random.normal(own_key, shape, jnp.float32) * deviation
    if len(cuts) > 0:
        values = level_of(own_key, shape, cuts, -0.22, 0.18) * values
    return jnp.clip(values, min=-limit, max=limit).astype(kind)


def setup_inputs(seed: int = 0, part: int = 0) -> dict:
    arg_keys = jax.random.split(jax.random.key(seed), 8)
    own_keys = jax.random.split(jax.random.fold_in(arg_keys[7], part), 8)
    return {
        "prompt_keys": draw_prompt_keys(jax.random.fold_in(jax.random.fold_in(arg_keys[7], part), 71), part),
        "prompt_values": bell_draw(own_keys[1], (PROMPT, KV_HEADS * HEAD_DIM), 1.0, 6.0, ((0, 16),)),
        "queries": draw_queries(jax.random.fold_in(jax.random.fold_in(arg_keys[7], part), 71), part),
        "resp_keys": bell_draw(own_keys[3], (2, RESP, KV_HEADS * HEAD_DIM), 1.0, 6.0, ((1, 16),)),
        "resp_values": bell_draw(own_keys[4], (2, RESP, KV_HEADS * HEAD_DIM), 1.0, 6.0, ((1, 16),)),
        "cotangent": jnp.clip(jax.random.uniform(own_keys[5], (2, RESP, HEADS * HEAD_DIM), jnp.float32, -48.0, 48.0) * level_of(own_keys[5], (2, RESP, HEADS * HEAD_DIM), ((1, 16),), -0.4, 0.0), -48.0, 48.0).astype(jnp.bfloat16),
        "lengths": draw_lengths(jax.random.fold_in(jax.random.fold_in(arg_keys[7], part), 71), part),
    }


def rounded(array):
    return lax.optimization_barrier(array.astype(jnp.bfloat16)).astype(jnp.float32)


def one_branch(query_rows, cotangent_rows, key_rows, value_rows, length):
    group_size = HEADS // KV_HEADS
    score_scale = HEAD_DIM ** -0.5
    total_keys = key_rows.shape[0]
    keys_all = key_rows.reshape(total_keys, KV_HEADS, HEAD_DIM).astype(jnp.float32)
    values_all = value_rows.reshape(total_keys, KV_HEADS, HEAD_DIM).astype(jnp.float32)
    key_positions = jnp.arange(total_keys, dtype=jnp.int32) - PROMPT
    height = math.gcd(RESP, 256)
    number = RESP // height
    query_blocks = query_rows.reshape(number, height, KV_HEADS, group_size, HEAD_DIM)
    cotangent_blocks = cotangent_rows.reshape(number, height, KV_HEADS, group_size, HEAD_DIM)

    def advance(carried, element):
        key_sum, value_sum = carried
        queries, upstream, block_index = element
        positions = block_index * height + jnp.arange(height, dtype=jnp.int32)
        live_rows = positions < length
        queries = queries.astype(jnp.float32)
        upstream = jnp.where(live_rows[:, None, None, None], upstream.astype(jnp.float32), 0.0)
        scores = jnp.einsum("qkgd,nkd->kgqn", queries, keys_all) * score_scale
        scores = jnp.where(key_positions[None, :] <= positions[:, None], scores, -jnp.inf)
        log_norm = jax.nn.logsumexp(scores, axis=-1)
        probs = jnp.exp(scores - log_norm[..., None])
        probs_low = rounded(probs)
        attended = jnp.einsum("kgqn,nkd->kgqd", probs_low, values_all)
        attended = rounded(jnp.where(live_rows[None, None, :, None], attended, 0.0))
        delta = jnp.einsum("qkgd,kgqd->kgq", upstream, attended)
        prob_grad = jnp.einsum("qkgd,nkd->kgqn", upstream, values_all)
        score_grad = rounded(probs * (prob_grad - delta[..., None]))
        query_grad = jnp.einsum("kgqn,nkd->qkgd", score_grad, keys_all) * score_scale
        key_sum = key_sum + jnp.einsum("kgqn,qkgd->nkd", score_grad, queries) * score_scale
        value_sum = value_sum + jnp.einsum("kgqn,qkgd->nkd", probs_low, upstream)
        return (key_sum, value_sum), query_grad.reshape(height, HEADS * HEAD_DIM)

    empty_sum = jnp.zeros((total_keys, KV_HEADS, HEAD_DIM), jnp.float32)
    indices = jnp.arange(number, dtype=jnp.int32)
    (key_sum, value_sum), query_grads = lax.scan(advance, (empty_sum, empty_sum), (query_blocks, cotangent_blocks, indices))
    width = KV_HEADS * HEAD_DIM
    return query_grads.reshape(RESP, HEADS * HEAD_DIM), key_sum.reshape(total_keys, width), value_sum.reshape(total_keys, width)


def reference(prompt_keys, prompt_values, queries, resp_keys, resp_values, cotangent, lengths):
    query_grads = []
    resp_key_grads = []
    resp_value_grads = []
    prompt_key_sum = jnp.zeros(prompt_keys.shape, jnp.float32)
    prompt_value_sum = jnp.zeros(prompt_values.shape, jnp.float32)
    for branch in range(2):
        key_rows = jnp.concatenate([prompt_keys, resp_keys[branch]], axis=0)
        value_rows = jnp.concatenate([prompt_values, resp_values[branch]], axis=0)
        grad_rows, key_grad, value_grad = one_branch(queries[branch], cotangent[branch], key_rows, value_rows, lengths[branch])
        query_grads.append(grad_rows)
        prompt_key_sum = prompt_key_sum + key_grad[:PROMPT]
        prompt_value_sum = prompt_value_sum + value_grad[:PROMPT]
        resp_key_grads.append(key_grad[PROMPT:])
        resp_value_grads.append(value_grad[PROMPT:])
    return (jnp.stack(query_grads), jnp.stack(resp_key_grads), jnp.stack(resp_value_grads), prompt_key_sum, prompt_value_sum)
```

```python
import functools

import jax
import jax.numpy as jnp
from jax import lax
from jax.experimental import pallas as pl
from jax.experimental.pallas import tpu as pltpu
from jax.sharding import PartitionSpec as P

HEAD_DIM = 128
SCALE = HEAD_DIM ** (-0.5)
LOG2E = 1.4426950408889634
MIB = 1024 * 1024


def chip_of(pos, n):
    high = pos // (n // 2)
    return (1 - high) * (2 * pos) + high * (2 * (n - 1 - pos) + 1)


def place(n):
    me = lax.axis_index("ctx")
    core, chip = me % 2, me // 2
    odd = chip % 2
    pos = (1 - odd) * (chip // 2) + odd * (n - 1 - chip // 2)
    partner = 2 * chip + 1 - core
    right = 2 * chip_of((pos + 1) % n, n) + core
    left = 2 * chip_of((pos + n - 1) % n, n) + core
    return core, chip, pos, partner, (right, left)


def greet(partner, sides):
    barrier = pltpu.get_barrier_semaphore()
    for other in (partner,) + sides:
        pl.semaphore_signal(
            barrier, inc=1, device_id={"ctx": other}, device_id_type=pl.DeviceIdType.MESH
        )
    pl.semaphore_wait(barrier, 3)


def steps_of(n):
    far, near = n // 2, n - 1 - n // 2
    return ((far, near), (near, far))


def remote(src, dst, send, recv, device):
    return pltpu.make_async_remote_copy(
        src_ref=src,
        dst_ref=dst,
        send_sem=send,
        recv_sem=recv,
        device_id={"ctx": device},
        device_id_type=pl.DeviceIdType.MESH,
    )


def gather_kernel(
    n, pk, pv, rk, rv, q, u, gpk, gpv, grk, grv, qp, up, send, recv, psend, precv, local_sem
):
    core, chip, pos, partner, sides = place(n)
    prows, rrows = pk.shape[0], rk.shape[1]
    width = pk.shape[1] // 2
    wide = q.shape[2] // 2
    hops = steps_of(n)
    mine = pl.ds(pl.multiple_of(core * width, width), width)
    theirs = pl.ds(pl.multiple_of((1 - core) * width, width), width)
    inputs = ((pk, rk), (pv, rv))
    gathered = ((gpk, grk), (gpv, grv))

    def spot(kind, part, where, source):
        ref = gathered[kind][part]
        if part == 0:
            start = where * 2 * prows + source * prows
            return ref.at[pl.ds(pl.multiple_of(start, prows), prows), :]
        start = where * 2 * rrows + source * rrows
        return ref.at[:, pl.ds(pl.multiple_of(start, 16), rrows), :]

    def columns(kind, part, cols):
        ref = inputs[kind][part]
        return ref.at[:, cols] if part == 0 else ref.at[:, :, cols]

    greet(partner, sides)
    swaps, locals_ = {}, []
    for kind in range(2):
        for part in range(2):
            swaps[kind, part] = remote(
                columns(kind, part, theirs), spot(kind, part, chip, core),
                psend.at[kind * 2 + part], precv.at[kind * 2 + part], partner,
            )
            swaps[kind, part].start()
    copies = {}

    def forward(t, piece, way, kind, part):
        hop_from = (pos + n - (t - 1)) % n if way == 0 else (pos + t - 1) % n
        where = chip_of(hop_from, n)
        source = core if piece == 0 else 1 - core
        dst = spot(kind, part, where, source)
        src = columns(kind, part, mine) if (t == 1 and piece == 0) else dst
        copy = remote(
            src, dst, send.at[way, kind * 2 + part, t - 1, piece],
            recv.at[way, kind * 2 + part, t - 1, piece], sides[way],
        )
        copy.start()
        copies[t, piece, way, kind, part] = copy

    for t in range(1, n // 2 + 1):
        for piece in range(2):
            for part in (1, 0):
                for way in range(2):
                    for kind in ((0, 1) if way == 0 else (1, 0)):
                        if t > hops[way][kind]:
                            continue
                        if t > 1:
                            copies[t - 1, piece, way, kind, part].wait_recv()
                        elif piece == 1 and way == 0:
                            swaps[kind, part].wait_recv()
                        forward(t, piece, way, kind, part)
        if t == 1:
            for kind in range(2):
                for part in range(2):
                    copy = pltpu.make_async_copy(
                        columns(kind, part, mine), spot(kind, part, chip, core),
                        local_sem.at[kind * 2 + part],
                    )
                    copy.start()
                    locals_.append(copy)
            other_wide = pl.ds(pl.multiple_of((1 - core) * wide, wide), wide)
            big = []
            for i, (src, dst) in enumerate(((q, qp), (u, up))):
                copy = remote(
                    src.at[:, :, other_wide], dst, psend.at[4 + i], precv.at[4 + i], partner
                )
                copy.start()
                big.append(copy)
    for (t, piece, way, kind, part), copy in copies.items():
        if t == hops[way][kind]:
            copy.wait_recv()
        copy.wait_send()
    for copy in swaps.values():
        copy.wait_send()
    for copy in locals_:
        copy.wait()
    for copy in big:
        copy.wait()


def compute_kernel(
    block, lengths, pk, pv, rk, rv, q, u, qp, up,
    dpk, dpv, drk, drv, dq_own, dq_far,
    qs, us, s_buf, d_buf, qt_buf, m_buf, l_buf, e_buf,
):
    me = lax.axis_index("ctx")
    core, chip = me % 2, me // 2
    rows = q.shape[1]
    wide = q.shape[2] // 2
    heads = pk.shape[1] // HEAD_DIM
    group = wide // HEAD_DIM // heads
    half = group * rows
    lanes = 2 * half
    prompt_blocks = pk.shape[0] // block
    base = chip * 2 * rows
    factor = SCALE * LOG2E
    resp_blocks = ((chip + 1) * 2 * rows + block - 1) // block
    dpk[...] = jnp.zeros_like(dpk)
    dpv[...] = jnp.zeros_like(dpv)
    drk[...] = jnp.zeros_like(drk)
    drv[...] = jnp.zeros_like(drv)

    lane = lax.broadcasted_iota(jnp.int32, (1, lanes), 1)
    own_half = lane < half
    row_of = lax.rem(lane, rows)
    positions = base + row_of + rows * jnp.where(own_half, core, 1 - core)
    key_iota = lax.broadcasted_iota(jnp.int32, (block, 1), 0)
    row_iota = lax.broadcasted_iota(jnp.int32, (rows, 1), 0)
    nt = (((1,), (1,)), ((), ()))

    for b in range(2):
        length = lengths[b]
        live = base < length

        @pl.when(jnp.logical_not(live))
        def _():
            dq_own[b] = jnp.zeros(dq_own.shape[1:], jnp.float32)
            dq_far[b] = jnp.zeros(dq_far.shape[1:], jnp.float32)

        @pl.when(live)
        def _():
            @pl.loop(0, heads)
            def _(k):
                own_live = base + core * rows + row_iota < length
                far_live = base + (1 - core) * rows + row_iota < length
                for g in range(group):
                    near = pl.ds(pl.multiple_of(k * (group * HEAD_DIM) + g * HEAD_DIM, HEAD_DIM), HEAD_DIM)
                    full = pl.ds(pl.multiple_of(core * wide + k * (group * HEAD_DIM) + g * HEAD_DIM, HEAD_DIM), HEAD_DIM)
                    at = pl.ds(g * rows, rows)
                    to = pl.ds(half + g * rows, rows)
                    qs[at, :] = q[b, :, full]
                    qs[to, :] = qp[b, :, near]
                    mine = u[b, :, full]
                    us[at, :] = jnp.where(own_live, mine, jnp.zeros_like(mine))
                    far = up[b, :, near]
                    us[to, :] = jnp.where(far_live, far, jnp.zeros_like(far))
                cols = pl.ds(pl.multiple_of(k * HEAD_DIM, HEAD_DIM), HEAD_DIM)
                qq, uu = qs[...], us[...]

                def key_rows(j):
                    return pl.ds(pl.multiple_of(j * block, block), block)

                m_buf[...] = jnp.full_like(m_buf, -jnp.inf)
                l_buf[...] = jnp.zeros_like(l_buf)
                e_buf[...] = jnp.zeros_like(e_buf)
                qt_buf[...] = jnp.zeros_like(qt_buf)

                def scores(keys, at, j, causal):
                    s = lax.dot_general(keys, qq, nt, preferred_element_type=jnp.float32)
                    if causal:
                        s = jnp.where(key_iota + j * block <= positions, s, -jnp.inf)
                    s_buf[at, :] = s
                    m_buf[...] = jnp.maximum(m_buf[...], jnp.max(s, axis=0, keepdims=True))

                @pl.loop(0, prompt_blocks)
                def _(j):
                    scores(pk[key_rows(j), cols], key_rows(j), j, False)

                @pl.loop(0, resp_blocks)
                def _(j):
                    scores(rk[b, key_rows(j), cols], key_rows(prompt_blocks + j), j, True)

                shift = m_buf[...] * factor

                def weights(vals, at):
                    p = jnp.exp2(s_buf[at, :] * factor - shift)
                    d = lax.dot_general(vals, uu, nt, preferred_element_type=jnp.float32)
                    l_buf[...] += jnp.sum(p, axis=0, keepdims=True)
                    e_buf[...] += jnp.sum(p * d, axis=0, keepdims=True)
                    s_buf[at, :] = p
                    d_buf[at, :] = d

                @pl.loop(0, prompt_blocks)
                def _(j):
                    weights(pv[key_rows(j), cols], key_rows(j))

                @pl.loop(0, resp_blocks)
                def _(j):
                    weights(rv[b, key_rows(j), cols], key_rows(prompt_blocks + j))

                inverse = 1.0 / l_buf[...]
                delta = e_buf[...] * inverse

                def grads(keys, at):
                    p = s_buf[at, :] * inverse
                    ds = (p * (d_buf[at, :] - delta)).astype(jnp.bfloat16)
                    dv = jnp.dot(p.astype(jnp.bfloat16), uu, preferred_element_type=jnp.float32)
                    dk = jnp.dot(ds, qq, preferred_element_type=jnp.float32) * SCALE
                    qt_buf[...] += jnp.dot(keys.T, ds, preferred_element_type=jnp.float32)
                    return dk, dv

                @pl.loop(0, prompt_blocks)
                def _(j):
                    at = key_rows(j)
                    dk, dv = grads(pk[at, cols], at)
                    dpk[at, cols] += dk
                    dpv[at, cols] += dv

                @pl.loop(0, resp_blocks)
                def _(j):
                    at = key_rows(j)
                    dk, dv = grads(rk[b, at, cols], key_rows(prompt_blocks + j))
                    drk[b, at, cols] = dk
                    drv[b, at, cols] = dv

                dq = qt_buf[...].T * SCALE
                for g in range(group):
                    near = pl.ds(pl.multiple_of(k * (group * HEAD_DIM) + g * HEAD_DIM, HEAD_DIM), HEAD_DIM)
                    dq_own[b, :, near] = dq[g * rows : (g + 1) * rows]
                    dq_far[b, :, near] = dq[half + g * rows : half + (g + 1) * rows]


def scatter_kernel(
    n, dpk, dpv, drk, drv, dq_own, dq_far, gq, gpk, gpv, grk, grv,
    sp, sr, rp, rr, fp, fr, send, recv, psend, precv, local_sem,
):
    core, chip, pos, partner, sides = place(n)
    prows, rrows = gpk.shape[0], grk.shape[1]
    width = gpk.shape[1] // 2
    wide = dq_own.shape[2]
    hops = steps_of(n)
    mine = pl.ds(pl.multiple_of(core * width, width), width)
    mine_wide = pl.ds(pl.multiple_of(core * wide, wide), wide)
    terms = ((dpk, drk), (dpv, drv))
    sends, gets, finals = (sp, sr), (rp, rr), (fp, fr)

    greet(partner, sides)
    far = remote(dq_far, gq.at[:, :, mine_wide], psend.at[4], precv.at[4], partner)
    far.start()
    near = pltpu.make_async_copy(dq_own, gq.at[:, :, mine_wide], local_sem.at[0])
    near.start()

    def term(kind, part, where):
        ref = terms[kind][part]
        if part == 0:
            return ref[pl.ds(pl.multiple_of(where * 2 * prows, 2 * prows), 2 * prows), :]
        return ref[:, pl.ds(pl.multiple_of(where * 2 * rrows, 2 * rrows), 2 * rrows), :]

    copies = {}
    for t in range(1, n // 2 + 1):
        for part in (1, 0):
            for way in range(2):
                for kind in ((0, 1) if way == 0 else (1, 0)):
                    total = hops[way][kind]
                    if t > total:
                        continue
                    far_by = total - t + 1
                    target = (pos + far_by) % n if way == 0 else (pos + n - far_by) % n
                    value = term(kind, part, chip_of(target, n))
                    if t > 1:
                        copies[t - 1, way, kind, part].wait_recv()
                        value = value + gets[part][way, kind, t - 2].astype(jnp.float32)
                    sends[part][way, kind, t - 1] = value.astype(jnp.bfloat16)
                    copy = remote(
                        sends[part].at[way, kind, t - 1], gets[part].at[way, kind, t - 1],
                        send.at[way, kind * 2 + part, t - 1],
                        recv.at[way, kind * 2 + part, t - 1], sides[way],
                    )
                    copy.start()
                    copies[t, way, kind, part] = copy
    swaps = []
    outs = ((gpk, grk), (gpv, grv))
    for part in (1, 0):
        for kind in range(2):
            value = term(kind, part, chip)
            for way in range(2):
                last = hops[way][kind]
                copies[last, way, kind, part].wait_recv()
                value = value + gets[part][way, kind, last - 1].astype(jnp.float32)
            finals[part][kind] = value
            out = outs[kind][part]
            if part == 0:
                own_rows = pl.ds(pl.multiple_of(core * prows, prows), prows)
                far_rows = pl.ds(pl.multiple_of((1 - core) * prows, prows), prows)
                src, dst = fp.at[kind, far_rows, :], out.at[:, mine]
            else:
                own_rows = pl.ds(pl.multiple_of(core * rrows, 16), rrows)
                far_rows = pl.ds(pl.multiple_of((1 - core) * rrows, 16), rrows)
                src, dst = fr.at[kind, :, far_rows, :], out.at[:, :, mine]
            copy = remote(src, dst, psend.at[kind * 2 + part], precv.at[kind * 2 + part], partner)
            copy.start()
            swaps.append(copy)
            if part == 0:
                out[:, mine] = fp[kind, own_rows, :]
            else:
                out[:, :, mine] = fr[kind, :, own_rows, :]
    for copy in copies.values():
        copy.wait_send()
    for copy in swaps:
        copy.wait()
    far.wait()
    near.wait()


def key_block(prompt, resp):
    size = 256
    while prompt % size or resp % size:
        size //= 2
    return size


def local(prompt_keys, prompt_values, queries, resp_keys, resp_values, cotangent, lengths):
    devices = lax.axis_size("ctx")
    n = devices // 2
    prows, columns = prompt_keys.shape
    rows, wide = queries.shape[1], queries.shape[2] // 2
    width = columns // 2
    prompt, resp = prows * devices, rows * devices
    vmem = pl.BlockSpec(memory_space=pltpu.VMEM)
    smem = pl.BlockSpec(memory_space=pltpu.SMEM)
    hbm = pl.BlockSpec(memory_space=pl.ANY)
    shape = jax.ShapeDtypeStruct
    bf16, f32 = jnp.bfloat16, jnp.float32
    dma = pltpu.SemaphoreType.DMA
    hop = n // 2

    gpk, gpv, grk, grv, qp, up = pl.pallas_call(
        functools.partial(gather_kernel, n),
        out_shape=(
            shape((prompt, width), bf16), shape((prompt, width), bf16),
            shape((2, resp, width), bf16), shape((2, resp, width), bf16),
            shape((2, rows, wide), bf16), shape((2, rows, wide), bf16),
        ),
        in_specs=[vmem] * 4 + [hbm] * 2,
        out_specs=(vmem,) * 4 + (hbm,) * 2,
        scratch_shapes=[
            dma((2, 4, hop, 2)), dma((2, 4, hop, 2)), dma((6,)), dma((6,)), dma((4,)),
        ],
        compiler_params=pltpu.CompilerParams(
            collective_id=0, has_side_effects=True, vmem_limit_bytes=24 * MIB
        ),
        name="gather",
    )(prompt_keys, prompt_values, resp_keys, resp_values, queries, cotangent)

    block = key_block(prompt, resp)
    lanes = 2 * rows * (wide // HEAD_DIM) // (width // HEAD_DIM)
    total = prompt + resp
    dpk, dpv, drk, drv, dq_own, dq_far = pl.pallas_call(
        functools.partial(compute_kernel, block),
        out_shape=(
            shape((prompt, width), f32), shape((prompt, width), f32),
            shape((2, resp, width), f32), shape((2, resp, width), f32),
            shape((2, rows, wide), f32), shape((2, rows, wide), f32),
        ),
        in_specs=[smem] + [vmem] * 8,
        out_specs=(vmem,) * 6,
        scratch_shapes=[
            pltpu.VMEM((lanes, HEAD_DIM), bf16), pltpu.VMEM((lanes, HEAD_DIM), bf16),
            pltpu.VMEM((total, lanes), f32), pltpu.VMEM((total, lanes), f32),
            pltpu.VMEM((HEAD_DIM, lanes), f32),
            pltpu.VMEM((1, lanes), f32), pltpu.VMEM((1, lanes), f32), pltpu.VMEM((1, lanes), f32),
        ],
        compiler_params=pltpu.CompilerParams(vmem_limit_bytes=56 * MIB),
        name="compute",
    )(lengths, gpk, gpv, grk, grv, queries, cotangent, qp, up)

    return scatter(n, dpk, dpv, drk, drv, dq_own, dq_far, prows, rows)


def scatter(n, dpk, dpv, drk, drv, dq_own, dq_far, prows, rows):
    width, wide = dpk.shape[1], dq_own.shape[2]
    vmem = pl.BlockSpec(memory_space=pltpu.VMEM)
    hbm = pl.BlockSpec(memory_space=pl.ANY)
    shape = jax.ShapeDtypeStruct
    bf16, f32 = jnp.bfloat16, jnp.float32
    dma = pltpu.SemaphoreType.DMA
    hop = n // 2
    gq, gpk, gpv, grk, grv = pl.pallas_call(
        functools.partial(scatter_kernel, n),
        out_shape=(
            shape((2, rows, 2 * wide), f32),
            shape((prows, 2 * width), f32), shape((prows, 2 * width), f32),
            shape((2, rows, 2 * width), f32), shape((2, rows, 2 * width), f32),
        ),
        in_specs=[vmem] * 6,
        out_specs=(hbm,) + (vmem,) * 4,
        scratch_shapes=[
            pltpu.VMEM((2, 2, hop, 2 * prows, width), bf16),
            pltpu.VMEM((2, 2, hop, 2, 2 * rows, width), bf16),
            pltpu.VMEM((2, 2, hop, 2 * prows, width), bf16),
            pltpu.VMEM((2, 2, hop, 2, 2 * rows, width), bf16),
            pltpu.VMEM((2, 2 * prows, width), f32),
            pltpu.VMEM((2, 2, 2 * rows, width), f32),
            dma((2, 4, hop)), dma((2, 4, hop)), dma((5,)), dma((5,)), dma((1,)),
        ],
        compiler_params=pltpu.CompilerParams(
            collective_id=1, has_side_effects=True, vmem_limit_bytes=48 * MIB
        ),
        name="scatter",
    )(dpk, dpv, drk, drv, dq_own, dq_far)
    return gq, grk, grv, gpk, gpv


def solution(mesh):
    placed = (
        P(("pairs", "ctx"), None),
        P(("pairs", "ctx"), None),
        P("pairs", "ctx", None),
        P("pairs", "ctx", None),
        P("pairs", "ctx", None),
        P("pairs", "ctx", None),
        P("pairs"),
    )
    return jax.shard_map(
        local,
        mesh=mesh,
        in_specs=placed,
        out_specs=(
            P("pairs", "ctx", None),
            P("pairs", "ctx", None),
            P("pairs", "ctx", None),
            P(("pairs", "ctx"), None),
            P(("pairs", "ctx"), None),
        ),
        check_vma=False,
    )
```

```python
import functools

import jax
import jax.numpy as jnp
from jax import lax
from jax.experimental import pallas as pl
from jax.experimental.pallas import tpu as pltpu
from jax.sharding import PartitionSpec as P

HEAD_DIM = 128
SCALE = HEAD_DIM ** (-0.5)
LOG2E = 1.4426950408889634
MIB = 1024 * 1024


def chip_of(pos, n):
    high = pos // (n // 2)
    return (1 - high) * (2 * pos) + high * (2 * (n - 1 - pos) + 1)


def place(n):
    me = lax.axis_index("ctx")
    core, chip = me % 2, me // 2
    odd = chip % 2
    pos = (1 - odd) * (chip // 2) + odd * (n - 1 - chip // 2)
    partner = 2 * chip + 1 - core
    right = 2 * chip_of((pos + 1) % n, n) + core
    left = 2 * chip_of((pos + n - 1) % n, n) + core
    return core, chip, pos, partner, (right, left)


def greet(partner, sides):
    barrier = pltpu.get_barrier_semaphore()
    for other in (partner,) + sides:
        pl.semaphore_signal(
            barrier, inc=1, device_id={"ctx": other}, device_id_type=pl.DeviceIdType.MESH
        )
    pl.semaphore_wait(barrier, 3)


def steps_of(n):
    far, near = n // 2, n - 1 - n // 2
    return ((far, near), (near, far))


def remote(src, dst, send, recv, device):
    return pltpu.make_async_remote_copy(
        src_ref=src,
        dst_ref=dst,
        send_sem=send,
        recv_sem=recv,
        device_id={"ctx": device},
        device_id_type=pl.DeviceIdType.MESH,
    )


def fused_kernel(
    n, block, lengths, pk, pv, rk, rv, q, u,
    gq, grk, grv, gpk, gpv,
    kp, kr, qh, uh, qs, us, s_buf, d_buf, qt_buf, m_buf, l_buf, e_buf,
    tp, tr, sp, sr, rp, rr, fp, fr, dq,
    gsend, grecv, ssend, srecv, isend, irecv, ilocal, qsend, qrecv, qlocal,
    osend, orecv, olocal,
):
    core, chip, pos, partner, sides = place(n)
    prows, rrows = pk.shape[0], rk.shape[1]
    wide = q.shape[2] // 2
    heads = kp.shape[1]
    group = wide // HEAD_DIM // heads
    units = [(k, b) for k in range(heads) for b in range(2)]
    hops = steps_of(n)
    flows = ((0, 0), (1, 1), (0, 1), (1, 0))
    inputs = ((pk, rk), (pv, rv))
    outputs = ((gpk, grk), (gpv, grv))

    def head_columns(owner, k):
        return pl.ds(pl.multiple_of((owner * heads + k) * HEAD_DIM, HEAD_DIM), HEAD_DIM)

    def parts_in(unit):
        return (0, 1) if units[unit][1] == 0 else (1,)

    def parts_out(unit):
        return (1,) if units[unit][1] == 0 else (0, 1)

    def rows_of(where, size):
        return pl.ds(pl.multiple_of(where * size, 16), size)

    def gathered(kind, unit, part, rows):
        k, b = units[unit]
        return kp.at[kind, k, rows, :] if part == 0 else kr.at[kind, k, b, rows, :]

    def given(kind, unit, part, cols):
        ref = inputs[kind][part]
        return ref.at[:, cols] if part == 0 else ref.at[units[unit][1], :, cols]

    greet(partner, sides)
    entries = []
    for unit in range(len(units)):
        k = units[unit][0]
        for part in parts_in(unit):
            size = prows if part == 0 else rrows
            own = rows_of(chip * 2 + core, size)
            for kind in range(2):
                at = (kind, unit, part)
                away = remote(
                    given(kind, unit, part, head_columns(1 - core, k)),
                    gathered(kind, unit, part, own), isend.at[at], irecv.at[at], partner,
                )
                away.start()
                stay = pltpu.make_async_copy(
                    given(kind, unit, part, head_columns(core, k)),
                    gathered(kind, unit, part, own), ilocal.at[at],
                )
                stay.start()
                entries.append((unit, away, stay))
    wide_own = pl.ds(pl.multiple_of(core * wide, wide), wide)
    wide_far = pl.ds(pl.multiple_of((1 - core) * wide, wide), wide)
    query_moves = []
    for i, (src, dst) in enumerate(((q, qh), (u, uh))):
        away = remote(src.at[:, :, wide_far], dst.at[1], qsend.at[i], qrecv.at[i], partner)
        away.start()
        stay = pltpu.make_async_copy(src.at[:, :, wide_own], dst.at[0], qlocal.at[i])
        stay.start()
        query_moves += [away, stay]

    moved = {}

    def pull(unit, t):
        if t == 1:
            for owner, away, stay in entries:
                if owner == unit:
                    away.wait_recv()
                    stay.wait()
        for part in parts_in(unit):
            size = 2 * (prows if part == 0 else rrows)
            for way, kind in flows:
                if t > hops[way][kind]:
                    continue
                if t > 1:
                    moved[unit, t - 1, part, way, kind].wait_recv()
                origin = (pos + n - (t - 1)) % n if way == 0 else (pos + t - 1) % n
                ref = gathered(kind, unit, part, rows_of(chip_of(origin, n), size))
                at = (way, kind, unit, part, t - 1)
                copy = remote(ref, ref, gsend.at[at], grecv.at[at], sides[way])
                copy.start()
                moved[unit, t, part, way, kind] = copy

    def pulled(unit):
        for part in parts_in(unit):
            for way, kind in flows:
                moved[unit, hops[way][kind], part, way, kind].wait_recv()

    sent = {}

    def term(kind, unit, part, where):
        k, b = units[unit]
        if part == 0:
            return tp[kind, k, rows_of(where, 2 * prows), :]
        return tr[kind, k, b, rows_of(where, 2 * rrows), :]

    def slot(bufs, part, way, kind, unit, t):
        k = units[unit][0]
        if part == 0:
            return bufs[0].at[way, kind, k, t - 1]
        return bufs[1].at[way, kind, unit, t - 1]

    def push(unit, t, part):
        for way, kind in flows:
            total = hops[way][kind]
            if t > total:
                continue
            away = total - t + 1
            target = (pos + away) % n if way == 0 else (pos + n - away) % n
            value = term(kind, unit, part, chip_of(target, n))
            if t > 1:
                sent[unit, t - 1, part, way, kind].wait_recv()
                value = value + slot((rp, rr), part, way, kind, unit, t - 1)[...].astype(jnp.float32)
            src = slot((sp, sr), part, way, kind, unit, t)
            src[...] = value.astype(jnp.bfloat16)
            at = (way, kind, unit, part, t - 1)
            copy = remote(
                src, slot((rp, rr), part, way, kind, unit, t), ssend.at[at], srecv.at[at], sides[way]
            )
            copy.start()
            sent[unit, t, part, way, kind] = copy

    outgoing = []

    def finish(unit, part):
        k, b = units[unit]
        size = prows if part == 0 else rrows
        for kind in range(2):
            value = term(kind, unit, part, chip)
            for way in range(2):
                last = hops[way][kind]
                sent[unit, last, part, way, kind].wait_recv()
                value = value + slot((rp, rr), part, way, kind, unit, last)[...].astype(jnp.float32)
            final = fp.at[kind, k] if part == 0 else fr.at[kind, k, b]
            final[...] = value
            out = outputs[kind][part]
            cols = head_columns(core, k)
            dst = out.at[:, cols] if part == 0 else out.at[b, :, cols]
            at = (kind, unit, part)
            away = remote(
                final.at[rows_of(1 - core, size), :], dst, osend.at[at], orecv.at[at], partner
            )
            away.start()
            stay = pltpu.make_async_copy(final.at[rows_of(core, size), :], dst, olocal.at[at])
            stay.start()
            outgoing.extend((away, stay))

    half = group * rrows
    lanes = 2 * half
    prompt_blocks = kp.shape[2] // block
    resp_blocks = kr.shape[3] // block
    base = chip * 2 * rrows
    factor = SCALE * LOG2E
    lane = lax.broadcasted_iota(jnp.int32, (1, lanes), 1)
    row_of = lax.rem(lane, rrows)
    positions = base + row_of + rrows * jnp.where(lane < half, core, 1 - core)
    key_iota = lax.broadcasted_iota(jnp.int32, (block, 1), 0)
    row_iota = lax.broadcasted_iota(jnp.int32, (rrows, 1), 0)
    nt = (((1,), (1,)), ((), ()))

    def key_rows(j):
        return pl.ds(pl.multiple_of(j * block, block), block)

    def compute(unit, ticks):
        k, b = units[unit]
        length = lengths[b]
        for source in range(2):
            owner = core if source == 0 else 1 - core
            live = base + owner * rrows + row_iota < length
            for g in range(group):
                cols = pl.ds((k * group + g) * HEAD_DIM, HEAD_DIM)
                at = pl.ds(source * half + g * rrows, rrows)
                qs[at, :] = qh[source, b, :, cols]
                rows = uh[source, b, :, cols]
                us[at, :] = jnp.where(live, rows, jnp.zeros_like(rows))
        m_buf[...] = jnp.full_like(m_buf, -jnp.inf)
        l_buf[...] = jnp.zeros_like(l_buf)
        e_buf[...] = jnp.zeros_like(e_buf)
        qt_buf[...] = jnp.zeros_like(qt_buf)
        ticks(0)

        def scores(keys, at, j, causal):
            s = lax.dot_general(keys, qs[...], nt, preferred_element_type=jnp.float32)
            if causal:
                s = jnp.where(key_iota + j * block <= positions, s, -jnp.inf)
            s_buf[at, :] = s
            m_buf[...] = jnp.maximum(m_buf[...], jnp.max(s, axis=0, keepdims=True))

        @pl.loop(0, prompt_blocks)
        def _(j):
            scores(kp[0, k, key_rows(j), :], key_rows(j), j, False)

        ticks(1)

        @pl.loop(0, resp_blocks)
        def _(j):
            scores(kr[0, k, b, key_rows(j), :], key_rows(prompt_blocks + j), j, True)

        ticks(2)
        shift = m_buf[...] * factor

        def weights(vals, at):
            p = jnp.exp2(s_buf[at, :] * factor - shift)
            d = lax.dot_general(vals, us[...], nt, preferred_element_type=jnp.float32)
            l_buf[...] += jnp.sum(p, axis=0, keepdims=True)
            e_buf[...] += jnp.sum(p * d, axis=0, keepdims=True)
            s_buf[at, :] = p
            d_buf[at, :] = d

        @pl.loop(0, prompt_blocks)
        def _(j):
            weights(kp[1, k, key_rows(j), :], key_rows(j))

        ticks(3)

        @pl.loop(0, resp_blocks)
        def _(j):
            weights(kr[1, k, b, key_rows(j), :], key_rows(prompt_blocks + j))

        ticks(4)
        inverse = 1.0 / l_buf[...]
        delta = e_buf[...] * inverse

        def grads(keys, at):
            p = s_buf[at, :] * inverse
            ds = (p * (d_buf[at, :] - delta)).astype(jnp.bfloat16)
            dv = jnp.dot(p.astype(jnp.bfloat16), us[...], preferred_element_type=jnp.float32)
            dk = jnp.dot(ds, qs[...], preferred_element_type=jnp.float32) * SCALE
            qt_buf[...] += jnp.dot(keys.T, ds, preferred_element_type=jnp.float32)
            return dk, dv

        @pl.loop(0, prompt_blocks)
        def _(j):
            at = key_rows(j)
            pair = grads(kp[0, k, at, :], at)
            for kind in range(2):
                if b == 0:
                    tp[kind, k, at, :] = pair[kind]
                else:
                    tp[kind, k, at, :] += pair[kind]

        ticks(5)

        @pl.loop(0, resp_blocks)
        def _(j):
            at = key_rows(j)
            pair = grads(kr[0, k, b, at, :], key_rows(prompt_blocks + j))
            for kind in range(2):
                tr[kind, k, b, at, :] = pair[kind]

        ticks(6)
        result = qt_buf[...].T * SCALE
        for source in range(2):
            for g in range(group):
                start = source * half + g * rrows
                dq[source, b, :, pl.ds((k * group + g) * HEAD_DIM, HEAD_DIM)] = result[
                    start : start + rrows
                ]
        span = group * HEAD_DIM
        cols = pl.ds(k * span, span)
        to = pl.ds(pl.multiple_of(core * wide + k * span, span), span)
        i = 2 + unit
        away = remote(dq.at[1, b, :, cols], gq.at[b, :, to], qsend.at[i], qrecv.at[i], partner)
        away.start()
        stay = pltpu.make_async_copy(dq.at[0, b, :, cols], gq.at[b, :, to], qlocal.at[i])
        stay.start()
        outgoing.extend((away, stay))

    last = len(units) - 1
    far = n // 2
    pulls = [(unit, t) for unit in range(1, last + 1) for t in range(1, far + 1)]

    def advance(count):
        for _ in range(min(count, len(pulls))):
            pull(*pulls.pop(0))

    pull(0, 1)
    for copy in query_moves:
        copy.wait()
    for t in range(2, far + 1):
        pull(0, t)
        advance(1)
    pulled(0)

    for unit in range(last + 1):
        pushes = []
        if unit > 0:
            pushes = [(unit - 1, t) for t in range(1, far + 1)]

        def ticks(at, unit=unit, pushes=pushes):
            due = -(-far // 3)
            if at in (0, 2, 4, 6):
                for _ in range(-(-far // 4)):
                    if pushes:
                        which, t = pushes.pop(0)
                        for part in reversed(parts_out(which)):
                            push(which, t, part)
            if at in (1, 3, 5):
                advance(due)
            if at == 0 and unit > 1:
                for part in parts_out(unit - 2):
                    finish(unit - 2, part)
            if at == 5 and unit == last:
                push(unit, 1, 0)

        compute(unit, ticks)
        if unit < last:
            while pulls and pulls[0][0] <= unit + 1:
                advance(1)
            pulled(unit + 1)
    for t in range(1, far + 1):
        push(last, t, 1)
        if t > 1:
            push(last, t, 0)
        if t == 1:
            for part in parts_out(last - 1):
                finish(last - 1, part)
    finish(last, 0)
    finish(last, 1)
    for copy in moved.values():
        copy.wait_send()
    for copy in sent.values():
        copy.wait_send()
    for _, away, _ in entries:
        away.wait_send()
    for copy in outgoing:
        copy.wait()


def key_block(prompt, resp):
    size = 256
    while prompt % size or resp % size:
        size //= 2
    return size


def local(prompt_keys, prompt_values, queries, resp_keys, resp_values, cotangent, lengths):
    devices = lax.axis_size("ctx")
    n = devices // 2
    prows, columns = prompt_keys.shape
    rows, wide = queries.shape[1], queries.shape[2] // 2
    heads = columns // 2 // HEAD_DIM
    prompt, resp = prows * devices, rows * devices
    smem = pl.BlockSpec(memory_space=pltpu.SMEM)
    hbm = pl.BlockSpec(memory_space=pl.ANY)
    shape = jax.ShapeDtypeStruct
    bf16, f32 = jnp.bfloat16, jnp.float32
    vmem, dma = pltpu.VMEM, pltpu.SemaphoreType.DMA
    hop, units = n // 2, 2 * heads
    block = key_block(prompt, resp)
    lanes = 2 * rows * (wide // HEAD_DIM) // heads
    total = prompt + resp
    gq, grk, grv, gpk, gpv = pl.pallas_call(
        functools.partial(fused_kernel, n, block),
        out_shape=(
            shape((2, rows, 2 * wide), f32),
            shape((2, rows, columns), f32), shape((2, rows, columns), f32),
            shape((prows, columns), f32), shape((prows, columns), f32),
        ),
        in_specs=[smem] + [hbm] * 6,
        out_specs=(hbm,) * 5,
        scratch_shapes=[
            vmem((2, heads, prompt, HEAD_DIM), bf16),
            vmem((2, heads, 2, resp, HEAD_DIM), bf16),
            vmem((2, 2, rows, wide), bf16), vmem((2, 2, rows, wide), bf16),
            vmem((lanes, HEAD_DIM), bf16), vmem((lanes, HEAD_DIM), bf16),
            vmem((total, lanes), f32), vmem((total, lanes), f32),
            vmem((HEAD_DIM, lanes), f32),
            vmem((1, lanes), f32), vmem((1, lanes), f32), vmem((1, lanes), f32),
            vmem((2, heads, prompt, HEAD_DIM), f32),
            vmem((2, heads, 2, resp, HEAD_DIM), f32),
            vmem((2, 2, heads, hop, 2 * prows, HEAD_DIM), bf16),
            vmem((2, 2, units, hop, 2 * rows, HEAD_DIM), bf16),
            vmem((2, 2, heads, hop, 2 * prows, HEAD_DIM), bf16),
            vmem((2, 2, units, hop, 2 * rows, HEAD_DIM), bf16),
            vmem((2, heads, 2 * prows, HEAD_DIM), f32),
            vmem((2, heads, 2, 2 * rows, HEAD_DIM), f32),
            vmem((2, 2, rows, wide), f32),
            dma((2, 2, units, 2, hop)), dma((2, 2, units, 2, hop)),
            dma((2, 2, units, 2, hop)), dma((2, 2, units, 2, hop)),
            dma((2, units, 2)), dma((2, units, 2)), dma((2, units, 2)),
            dma((2 + units,)), dma((2 + units,)), dma((2 + units,)),
            dma((2, units, 2)), dma((2, units, 2)), dma((2, units, 2)),
        ],
        compiler_params=pltpu.CompilerParams(
            collective_id=0, has_side_effects=True, vmem_limit_bytes=60 * MIB
        ),
        name="fused",
    )(lengths, prompt_keys, prompt_values, resp_keys, resp_values, queries, cotangent)
    return gq, grk, grv, gpk, gpv


def solution(mesh):
    placed = (
        P(("pairs", "ctx"), None),
        P(("pairs", "ctx"), None),
        P("pairs", "ctx", None),
        P("pairs", "ctx", None),
        P("pairs", "ctx", None),
        P("pairs", "ctx", None),
        P("pairs"),
    )
    return jax.shard_map(
        local,
        mesh=mesh,
        in_specs=placed,
        out_specs=(
            P("pairs", "ctx", None),
            P("pairs", "ctx", None),
            P("pairs", "ctx", None),
            P(("pairs", "ctx"), None),
            P(("pairs", "ctx"), None),
        ),
        check_vma=False,
    )
```

```python
import functools

import jax
import jax.numpy as jnp
from jax import lax
from jax.experimental import pallas as pl
from jax.experimental.pallas import tpu as pltpu
from jax.sharding import PartitionSpec as P

HEAD_DIM = 128
SCALE = HEAD_DIM ** (-0.5)
LOG2E = 1.4426950408889634
MIB = 1024 * 1024
TICKS = 7


def chip_of(pos, n):
    high = pos // (n // 2)
    return (1 - high) * (2 * pos) + high * (2 * (n - 1 - pos) + 1)


def place(n):
    me = lax.axis_index("ctx")
    core, chip = me % 2, me // 2
    odd = chip % 2
    pos = (1 - odd) * (chip // 2) + odd * (n - 1 - chip // 2)
    partner = 2 * chip + 1 - core
    right = 2 * chip_of((pos + 1) % n, n) + core
    left = 2 * chip_of((pos + n - 1) % n, n) + core
    return core, chip, pos, partner, (right, left)


def greet(partner, sides):
    barrier = pltpu.get_barrier_semaphore()
    for other in (partner,) + sides:
        pl.semaphore_signal(
            barrier, inc=1, device_id={"ctx": other}, device_id_type=pl.DeviceIdType.MESH
        )
    pl.semaphore_wait(barrier, 3)


def steps_of(n):
    far, near = n // 2, n - 1 - n // 2
    return ((far, near), (near, far))


def remote(src, dst, send, recv, device):
    return pltpu.make_async_remote_copy(
        src_ref=src,
        dst_ref=dst,
        send_sem=send,
        recv_sem=recv,
        device_id={"ctx": device},
        device_id_type=pl.DeviceIdType.MESH,
    )


def fused_kernel(
    n, block, lengths, pk, pv, rk, rv, q, u,
    gq, grk, grv, gpk, gpv,
    kp, kr, qh, uh, qs, us, s_buf, d_buf, qt_buf, m_buf, l_buf, e_buf,
    tp, tr, sp, sr, rp, rr, fp, fr, dq,
    gsend, grecv, ssend, srecv, isend, irecv, ilocal, qsend, qrecv, qlocal,
    osend, orecv, olocal,
):
    core, chip, pos, partner, sides = place(n)
    prows, rrows = pk.shape[0], rk.shape[1]
    wide = q.shape[2] // 2
    heads = kp.shape[1]
    group = wide // HEAD_DIM // heads
    units = [(k, b) for k in range(heads) for b in range(2)]
    hops = steps_of(n)
    flows = ((0, 0), (1, 1), (0, 1), (1, 0))
    inputs = ((pk, rk), (pv, rv))
    outputs = ((gpk, grk), (gpv, grv))

    def head_columns(owner, k):
        return pl.ds(pl.multiple_of((owner * heads + k) * HEAD_DIM, HEAD_DIM), HEAD_DIM)

    def parts_in(unit):
        return (0, 1) if units[unit][1] == 0 else (1,)

    def parts_out(unit):
        return (1,) if units[unit][1] == 0 else (0, 1)

    def rows_of(where, size):
        return pl.ds(pl.multiple_of(where * size, 16), size)

    def gathered(kind, unit, part, rows):
        k, b = units[unit]
        return kp.at[kind, k, rows, :] if part == 0 else kr.at[kind, k, b, rows, :]

    def given(kind, unit, part, cols):
        ref = inputs[kind][part]
        return ref.at[:, cols] if part == 0 else ref.at[units[unit][1], :, cols]

    greet(partner, sides)
    entries = []
    for unit in range(len(units)):
        k = units[unit][0]
        for part in parts_in(unit):
            size = prows if part == 0 else rrows
            own = rows_of(chip * 2 + core, size)
            for kind in range(2):
                at = (kind, unit, part)
                away = remote(
                    given(kind, unit, part, head_columns(1 - core, k)),
                    gathered(kind, unit, part, own), isend.at[at], irecv.at[at], partner,
                )
                away.start()
                stay = pltpu.make_async_copy(
                    given(kind, unit, part, head_columns(core, k)),
                    gathered(kind, unit, part, own), ilocal.at[at],
                )
                stay.start()
                entries.append((unit, away, stay))
    wide_own = pl.ds(pl.multiple_of(core * wide, wide), wide)
    wide_far = pl.ds(pl.multiple_of((1 - core) * wide, wide), wide)
    query_moves = []
    for i, (src, dst) in enumerate(((q, qh), (u, uh))):
        away = remote(src.at[:, :, wide_far], dst.at[1], qsend.at[i], qrecv.at[i], partner)
        away.start()
        stay = pltpu.make_async_copy(src.at[:, :, wide_own], dst.at[0], qlocal.at[i])
        stay.start()
        query_moves += [away, stay]

    moved = {}

    def pull(unit, t):
        if t == 1:
            for owner, away, stay in entries:
                if owner == unit:
                    away.wait_recv()
                    stay.wait()
        for part in parts_in(unit):
            size = 2 * (prows if part == 0 else rrows)
            for way, kind in flows:
                if t > hops[way][kind]:
                    continue
                if t > 1:
                    moved[unit, t - 1, part, way, kind].wait_recv()
                origin = (pos + n - (t - 1)) % n if way == 0 else (pos + t - 1) % n
                ref = gathered(kind, unit, part, rows_of(chip_of(origin, n), size))
                at = (way, kind, unit, part, t - 1)
                copy = remote(ref, ref, gsend.at[at], grecv.at[at], sides[way])
                copy.start()
                moved[unit, t, part, way, kind] = copy

    def pulled(unit):
        for part in parts_in(unit):
            for way, kind in flows:
                moved[unit, hops[way][kind], part, way, kind].wait_recv()

    sent = {}

    def term(kind, unit, part, where):
        k, b = units[unit]
        if part == 0:
            return tp[kind, k, rows_of(where, 2 * prows), :]
        return tr[kind, k, b, rows_of(where, 2 * rrows), :]

    def slot(bufs, part, way, kind, unit, t):
        k = units[unit][0]
        if part == 0:
            return bufs[0].at[way, kind, k, t - 1]
        return bufs[1].at[way, kind, unit, t - 1]

    def push(unit, t, part):
        for way, kind in flows:
            total = hops[way][kind]
            if t > total:
                continue
            away = total - t + 1
            target = (pos + away) % n if way == 0 else (pos + n - away) % n
            value = term(kind, unit, part, chip_of(target, n))
            if t > 1:
                sent[unit, t - 1, part, way, kind].wait_recv()
                value = value + slot((rp, rr), part, way, kind, unit, t - 1)[...].astype(jnp.float32)
            src = slot((sp, sr), part, way, kind, unit, t)
            src[...] = value.astype(jnp.bfloat16)
            at = (way, kind, unit, part, t - 1)
            copy = remote(
                src, slot((rp, rr), part, way, kind, unit, t), ssend.at[at], srecv.at[at], sides[way]
            )
            copy.start()
            sent[unit, t, part, way, kind] = copy

    outgoing = []

    def finish(unit, part):
        k, b = units[unit]
        size = prows if part == 0 else rrows
        for kind in range(2):
            value = term(kind, unit, part, chip)
            for way in range(2):
                last = hops[way][kind]
                sent[unit, last, part, way, kind].wait_recv()
                value = value + slot((rp, rr), part, way, kind, unit, last)[...].astype(jnp.float32)
            final = fp.at[kind, k] if part == 0 else fr.at[kind, k, b]
            final[...] = value
            out = outputs[kind][part]
            cols = head_columns(core, k)
            dst = out.at[:, cols] if part == 0 else out.at[b, :, cols]
            at = (kind, unit, part)
            away = remote(
                final.at[rows_of(1 - core, size), :], dst, osend.at[at], orecv.at[at], partner
            )
            away.start()
            stay = pltpu.make_async_copy(final.at[rows_of(core, size), :], dst, olocal.at[at])
            stay.start()
            outgoing.extend((away, stay))

    half = group * rrows
    lanes = 2 * half
    prompt_blocks = kp.shape[2] // block
    resp_blocks = kr.shape[3] // block
    base = chip * 2 * rrows
    factor = SCALE * LOG2E
    lane = lax.broadcasted_iota(jnp.int32, (1, lanes), 1)
    row_of = lax.rem(lane, rrows)
    positions = base + row_of + rrows * jnp.where(lane < half, core, 1 - core)
    key_iota = lax.broadcasted_iota(jnp.int32, (block, 1), 0)
    row_iota = lax.broadcasted_iota(jnp.int32, (rrows, 1), 0)
    nt = (((1,), (1,)), ((), ()))

    def key_rows(j):
        return pl.ds(pl.multiple_of(j * block, block), block)

    def compute(unit, ticks):
        k, b = units[unit]
        length = lengths[b]
        for source in range(2):
            owner = core if source == 0 else 1 - core
            live = base + owner * rrows + row_iota < length
            for g in range(group):
                cols = pl.ds((k * group + g) * HEAD_DIM, HEAD_DIM)
                at = pl.ds(source * half + g * rrows, rrows)
                qs[at, :] = qh[source, b, :, cols]
                rows = uh[source, b, :, cols]
                us[at, :] = jnp.where(live, rows, jnp.zeros_like(rows))
        m_buf[...] = jnp.full_like(m_buf, -jnp.inf)
        l_buf[...] = jnp.zeros_like(l_buf)
        e_buf[...] = jnp.zeros_like(e_buf)
        qt_buf[...] = jnp.zeros_like(qt_buf)
        ticks(0)

        def scores(keys, at, j, causal):
            s = lax.dot_general(keys, qs[...], nt, preferred_element_type=jnp.float32)
            if causal:
                s = jnp.where(key_iota + j * block <= positions, s, -jnp.inf)
            s_buf[at, :] = s
            m_buf[...] = jnp.maximum(m_buf[...], jnp.max(s, axis=0, keepdims=True))

        @pl.loop(0, prompt_blocks, unroll=True)
        def _(j):
            scores(kp[0, k, key_rows(j), :], key_rows(j), j, False)

        ticks(1)

        @pl.loop(0, resp_blocks, unroll=True)
        def _(j):
            scores(kr[0, k, b, key_rows(j), :], key_rows(prompt_blocks + j), j, True)

        ticks(2)
        shift = m_buf[...] * factor

        def weights(vals, at):
            p = jnp.exp2(s_buf[at, :] * factor - shift)
            d = lax.dot_general(vals, us[...], nt, preferred_element_type=jnp.float32)
            l_buf[...] += jnp.sum(p, axis=0, keepdims=True)
            e_buf[...] += jnp.sum(p * d, axis=0, keepdims=True)
            s_buf[at, :] = p
            d_buf[at, :] = d

        @pl.loop(0, prompt_blocks, unroll=True)
        def _(j):
            weights(kp[1, k, key_rows(j), :], key_rows(j))

        ticks(3)

        @pl.loop(0, resp_blocks, unroll=True)
        def _(j):
            weights(kr[1, k, b, key_rows(j), :], key_rows(prompt_blocks + j))

        ticks(4)
        inverse = 1.0 / l_buf[...]
        delta = e_buf[...] * inverse

        def grads(keys, at):
            p = s_buf[at, :] * inverse
            ds = (p * (d_buf[at, :] - delta)).astype(jnp.bfloat16)
            dv = jnp.dot(p.astype(jnp.bfloat16), us[...], preferred_element_type=jnp.float32)
            dk = jnp.dot(ds, qs[...], preferred_element_type=jnp.float32) * SCALE
            qt_buf[...] += jnp.dot(keys.T, ds, preferred_element_type=jnp.float32)
            return dk, dv

        @pl.loop(0, prompt_blocks, unroll=True)
        def _(j):
            at = key_rows(j)
            pair = grads(kp[0, k, at, :], at)
            for kind in range(2):
                if b == 0:
                    tp[kind, k, at, :] = pair[kind]
                else:
                    tp[kind, k, at, :] += pair[kind]

        ticks(5)

        @pl.loop(0, resp_blocks, unroll=True)
        def _(j):
            at = key_rows(j)
            pair = grads(kr[0, k, b, at, :], key_rows(prompt_blocks + j))
            for kind in range(2):
                tr[kind, k, b, at, :] = pair[kind]

        ticks(6)
        result = qt_buf[...].T * SCALE
        for source in range(2):
            for g in range(group):
                start = source * half + g * rrows
                dq[source, b, :, pl.ds((k * group + g) * HEAD_DIM, HEAD_DIM)] = result[
                    start : start + rrows
                ]
        span = group * HEAD_DIM
        cols = pl.ds(k * span, span)
        to = pl.ds(pl.multiple_of(core * wide + k * span, span), span)
        i = 2 + unit
        away = remote(dq.at[1, b, :, cols], gq.at[b, :, to], qsend.at[i], qrecv.at[i], partner)
        away.start()
        stay = pltpu.make_async_copy(dq.at[0, b, :, cols], gq.at[b, :, to], qlocal.at[i])
        stay.start()
        outgoing.extend((away, stay))

    last = len(units) - 1
    far = n // 2
    pulls = [(w - t + 1, t) for w in range(last + far) for t in range(1, far + 1) if 0 <= w - t + 1 <= last]
    pulls.sort(key=lambda hop: (hop[0] + hop[1], hop[1]))

    def advance(count):
        for _ in range(min(count, len(pulls))):
            pull(*pulls.pop(0))

    first = pulls.index((0, far)) + 1
    advance(1)
    for copy in query_moves:
        copy.wait()
    advance(first - 1)
    pulled(0)
    per_tick = -(-len(pulls) // 6)
    due = {}
    for unit in range(last):
        for t in range(1, far + 1):
            when = (unit + 1) * TICKS + (t - 1) * 12 // far
            due.setdefault(min(when, (last + 1) * TICKS), []).append((unit, t))

    def push_all(unit, t):
        for part in reversed(parts_out(unit)):
            push(unit, t, part)
        if t == far:
            closing.append(unit)

    closing = []
    for unit in range(last + 1):

        def ticks(at, unit=unit):
            for which, t in due.get(unit * TICKS + at, []):
                push_all(which, t)
            if at > 0:
                advance(per_tick)
            if at == 5 and unit == last:
                push(unit, 1, 0)

        compute(unit, ticks)
        if unit < last:
            while any(hop[0] <= unit + 1 for hop in pulls):
                advance(1)
            pulled(unit + 1)
    push(last, 1, 1)
    for which, t in due.get((last + 1) * TICKS, []):
        push_all(which, t)
    for t in range(2, far + 1):
        push(last, t, 0)
        push(last, t, 1)
        if closing:
            which = closing.pop(0)
            for part in parts_out(which):
                finish(which, part)
    for which in closing:
        for part in parts_out(which):
            finish(which, part)
    finish(last, 0)
    finish(last, 1)
    for copy in moved.values():
        copy.wait_send()
    for copy in sent.values():
        copy.wait_send()
    for _, away, _ in entries:
        away.wait_send()
    for copy in outgoing:
        copy.wait()


def key_block(prompt, resp):
    size = 256
    while prompt % size or resp % size:
        size //= 2
    return size


def settle_kernel(*refs):
    count = (len(refs) - 2) // 3
    sources, targets, holds = refs[:count], refs[count : 2 * count], refs[2 * count : 3 * count]
    taken, given = refs[3 * count :]
    pieces = []
    for i, (source, target, hold) in enumerate(zip(sources, targets, holds)):
        chunks = 4 if source.size > 1 << 18 else 1
        step = source.shape[-1] // chunks
        for c in range(chunks):
            cut = (slice(None),) * (len(source.shape) - 1) + (pl.ds(c * step, step),)
            taking = pltpu.make_async_copy(source.at[cut], hold.at[cut], taken.at[i, c])
            taking.start()
            giving = pltpu.make_async_copy(hold.at[cut], target.at[cut], given.at[i, c])
            pieces.append((taking, giving))
    for taking, giving in pieces:
        taking.wait()
        giving.start()
    for _, giving in pieces:
        giving.wait()


def settle(*arrays):
    hbm = pl.BlockSpec(memory_space=pl.ANY)
    dma = pltpu.SemaphoreType.DMA
    return pl.pallas_call(
        settle_kernel,
        out_shape=tuple(jax.ShapeDtypeStruct(x.shape, x.dtype) for x in arrays),
        in_specs=[hbm] * len(arrays),
        out_specs=(hbm,) * len(arrays),
        scratch_shapes=[pltpu.VMEM(x.shape, x.dtype) for x in arrays]
        + [dma((len(arrays), 4)), dma((len(arrays), 4))],
        compiler_params=pltpu.CompilerParams(vmem_limit_bytes=60 * MIB),
        name="settle",
    )(*arrays)


def local(prompt_keys, prompt_values, queries, resp_keys, resp_values, cotangent, lengths):
    devices = lax.axis_size("ctx")
    n = devices // 2
    prows, columns = prompt_keys.shape
    rows, wide = queries.shape[1], queries.shape[2] // 2
    heads = columns // 2 // HEAD_DIM
    prompt, resp = prows * devices, rows * devices
    smem = pl.BlockSpec(memory_space=pltpu.SMEM)
    hbm = pl.BlockSpec(memory_space=pl.ANY)
    shape = jax.ShapeDtypeStruct
    bf16, f32 = jnp.bfloat16, jnp.float32
    vmem, dma = pltpu.VMEM, pltpu.SemaphoreType.DMA
    hop, units = n // 2, 2 * heads
    block = key_block(prompt, resp)
    lanes = 2 * rows * (wide // HEAD_DIM) // heads
    total = prompt + resp
    gq, grk, grv, gpk, gpv = pl.pallas_call(
        functools.partial(fused_kernel, n, block),
        out_shape=(
            shape((2, rows, 2 * wide), f32),
            shape((2, rows, columns), f32), shape((2, rows, columns), f32),
            shape((prows, columns), f32), shape((prows, columns), f32),
        ),
        in_specs=[smem] + [hbm] * 6,
        out_specs=(hbm,) * 5,
        scratch_shapes=[
            vmem((2, heads, prompt, HEAD_DIM), bf16),
            vmem((2, heads, 2, resp, HEAD_DIM), bf16),
            vmem((2, 2, rows, wide), bf16), vmem((2, 2, rows, wide), bf16),
            vmem((lanes, HEAD_DIM), bf16), vmem((lanes, HEAD_DIM), bf16),
            vmem((total, lanes), f32), vmem((total, lanes), f32),
            vmem((HEAD_DIM, lanes), f32),
            vmem((1, lanes), f32), vmem((1, lanes), f32), vmem((1, lanes), f32),
            vmem((2, heads, prompt, HEAD_DIM), f32),
            vmem((2, heads, 2, resp, HEAD_DIM), f32),
            vmem((2, 2, heads, hop, 2 * prows, HEAD_DIM), bf16),
            vmem((2, 2, units, hop, 2 * rows, HEAD_DIM), bf16),
            vmem((2, 2, heads, hop, 2 * prows, HEAD_DIM), bf16),
            vmem((2, 2, units, hop, 2 * rows, HEAD_DIM), bf16),
            vmem((2, heads, 2 * prows, HEAD_DIM), f32),
            vmem((2, heads, 2, 2 * rows, HEAD_DIM), f32),
            vmem((2, 2, rows, wide), f32),
            dma((2, 2, units, 2, hop)), dma((2, 2, units, 2, hop)),
            dma((2, 2, units, 2, hop)), dma((2, 2, units, 2, hop)),
            dma((2, units, 2)), dma((2, units, 2)), dma((2, units, 2)),
            dma((2 + units,)), dma((2 + units,)), dma((2 + units,)),
            dma((2, units, 2)), dma((2, units, 2)), dma((2, units, 2)),
        ],
        compiler_params=pltpu.CompilerParams(
            collective_id=0, has_side_effects=True, vmem_limit_bytes=60 * MIB
        ),
        name="fused",
    )(lengths, prompt_keys, prompt_values, resp_keys, resp_values, queries, cotangent)
    return settle(gq, grk, grv, gpk, gpv)


def solution(mesh):
    placed = (
        P(("pairs", "ctx"), None),
        P(("pairs", "ctx"), None),
        P("pairs", "ctx", None),
        P("pairs", "ctx", None),
        P("pairs", "ctx", None),
        P("pairs", "ctx", None),
        P("pairs"),
    )
    return jax.shard_map(
        local,
        mesh=mesh,
        in_specs=placed,
        out_specs=(
            P("pairs", "ctx", None),
            P("pairs", "ctx", None),
            P("pairs", "ctx", None),
            P(("pairs", "ctx"), None),
            P(("pairs", "ctx"), None),
        ),
        check_vma=False,
    )
```

```python
import functools

import jax
import jax.numpy as jnp
from jax import lax
from jax.experimental import pallas as pl
from jax.experimental.pallas import tpu as pltpu
from jax.sharding import PartitionSpec as P

HEAD_DIM = 128
SCALE = HEAD_DIM ** (-0.5)
LOG2E = 1.4426950408889634
MIB = 1024 * 1024
TICKS = 7


def chip_of(pos, n):
    high = pos // (n // 2)
    return (1 - high) * (2 * pos) + high * (2 * (n - 1 - pos) + 1)


def place(n):
    me = lax.axis_index("ctx")
    core, chip = me % 2, me // 2
    odd = chip % 2
    pos = (1 - odd) * (chip // 2) + odd * (n - 1 - chip // 2)
    partner = 2 * chip + 1 - core
    right = 2 * chip_of((pos + 1) % n, n) + core
    left = 2 * chip_of((pos + n - 1) % n, n) + core
    return core, chip, pos, partner, (right, left)


def greet(partner, sides):
    barrier = pltpu.get_barrier_semaphore()
    for other in (partner,) + sides:
        pl.semaphore_signal(
            barrier, inc=1, device_id={"ctx": other}, device_id_type=pl.DeviceIdType.MESH
        )
    pl.semaphore_wait(barrier, 3)


def steps_of(n):
    far, near = n // 2, n - 1 - n // 2
    return ((far, near), (near, far))


def remote(src, dst, send, recv, device):
    return pltpu.make_async_remote_copy(
        src_ref=src,
        dst_ref=dst,
        send_sem=send,
        recv_sem=recv,
        device_id={"ctx": device},
        device_id_type=pl.DeviceIdType.MESH,
    )


def fused_kernel(
    n, block, lengths, pk, pv, rk, rv, q, u,
    gq, grk, grv, gpk, gpv,
    kp, kr, qh, uh, qs, us, s_buf, d_buf, qt_buf, m_buf, l_buf, e_buf,
    tp, tr, sp, sr, rp, rr, fp, fr, dq,
    gsend, grecv, ssend, srecv, isend, irecv, ilocal, qsend, qrecv, qlocal,
    osend, orecv, olocal,
):
    core, chip, pos, partner, sides = place(n)
    prows, rrows = pk.shape[0], rk.shape[1]
    wide = q.shape[2] // 2
    heads = kp.shape[1]
    group = wide // HEAD_DIM // heads
    units = [(k, b) for k in range(heads) for b in range(2)]
    hops = steps_of(n)
    flows = ((0, 0), (1, 1), (0, 1), (1, 0))
    inputs = ((pk, rk), (pv, rv))
    outputs = ((gpk, grk), (gpv, grv))

    def head_columns(owner, k):
        return pl.ds(pl.multiple_of((owner * heads + k) * HEAD_DIM, HEAD_DIM), HEAD_DIM)

    def parts_in(unit):
        return (0, 1) if units[unit][1] == 0 else (1,)

    def parts_out(unit):
        return (1,) if units[unit][1] == 0 else (0, 1)

    def rows_of(where, size):
        return pl.ds(pl.multiple_of(where * size, 16), size)

    def gathered(kind, unit, part, rows):
        k, b = units[unit]
        return kp.at[kind, k, rows, :] if part == 0 else kr.at[kind, k, b, rows, :]

    def given(kind, unit, part, cols):
        ref = inputs[kind][part]
        return ref.at[:, cols] if part == 0 else ref.at[units[unit][1], :, cols]

    greet(partner, sides)
    entries = []
    for unit in range(len(units)):
        k = units[unit][0]
        for part in parts_in(unit):
            size = prows if part == 0 else rrows
            own = rows_of(chip * 2 + core, size)
            for kind in range(2):
                at = (kind, unit, part)
                away = remote(
                    given(kind, unit, part, head_columns(1 - core, k)),
                    gathered(kind, unit, part, own), isend.at[at], irecv.at[at], partner,
                )
                away.start()
                stay = pltpu.make_async_copy(
                    given(kind, unit, part, head_columns(core, k)),
                    gathered(kind, unit, part, own), ilocal.at[at],
                )
                stay.start()
                entries.append((unit, away, stay))
    wide_own = pl.ds(pl.multiple_of(core * wide, wide), wide)
    wide_far = pl.ds(pl.multiple_of((1 - core) * wide, wide), wide)
    query_moves = []
    for i, (src, dst) in enumerate(((q, qh), (u, uh))):
        away = remote(src.at[:, :, wide_far], dst.at[1], qsend.at[i], qrecv.at[i], partner)
        away.start()
        stay = pltpu.make_async_copy(src.at[:, :, wide_own], dst.at[0], qlocal.at[i])
        stay.start()
        query_moves += [away, stay]

    moved = {}

    def pull(unit, t):
        if t == 1:
            for owner, away, stay in entries:
                if owner == unit:
                    away.wait_recv()
                    stay.wait()
        for part in parts_in(unit):
            size = 2 * (prows if part == 0 else rrows)
            for way, kind in flows:
                if t > hops[way][kind]:
                    continue
                if t > 1:
                    moved[unit, t - 1, part, way, kind].wait_recv()
                origin = (pos + n - (t - 1)) % n if way == 0 else (pos + t - 1) % n
                ref = gathered(kind, unit, part, rows_of(chip_of(origin, n), size))
                at = (way, kind, unit, part, t - 1)
                copy = remote(ref, ref, gsend.at[at], grecv.at[at], sides[way])
                copy.start()
                moved[unit, t, part, way, kind] = copy

    def pulled(unit):
        for part in parts_in(unit):
            for way, kind in flows:
                moved[unit, hops[way][kind], part, way, kind].wait_recv()

    sent = {}

    def term(kind, unit, part, where):
        k, b = units[unit]
        if part == 0:
            return tp[kind, k, rows_of(where, 2 * prows), :]
        return tr[kind, k, b, rows_of(where, 2 * rrows), :]

    def slot(bufs, part, way, kind, unit, t):
        k = units[unit][0]
        if part == 0:
            return bufs[0].at[way, kind, k, t - 1]
        return bufs[1].at[way, kind, unit, t - 1]

    def push(unit, t, part):
        for way, kind in flows:
            total = hops[way][kind]
            if t > total:
                continue
            away = total - t + 1
            target = (pos + away) % n if way == 0 else (pos + n - away) % n
            value = term(kind, unit, part, chip_of(target, n))
            if t > 1:
                sent[unit, t - 1, part, way, kind].wait_recv()
                value = value + slot((rp, rr), part, way, kind, unit, t - 1)[...].astype(jnp.float32)
            src = slot((sp, sr), part, way, kind, unit, t)
            src[...] = value.astype(jnp.bfloat16)
            at = (way, kind, unit, part, t - 1)
            copy = remote(
                src, slot((rp, rr), part, way, kind, unit, t), ssend.at[at], srecv.at[at], sides[way]
            )
            copy.start()
            sent[unit, t, part, way, kind] = copy

    outgoing = []

    def finish(unit, part):
        k, b = units[unit]
        size = prows if part == 0 else rrows
        for kind in range(2):
            value = term(kind, unit, part, chip)
            for way in range(2):
                last = hops[way][kind]
                sent[unit, last, part, way, kind].wait_recv()
                value = value + slot((rp, rr), part, way, kind, unit, last)[...].astype(jnp.float32)
            final = fp.at[kind, k] if part == 0 else fr.at[kind, k, b]
            final[...] = value
            out = outputs[kind][part]
            cols = head_columns(core, k)
            dst = out.at[:, cols] if part == 0 else out.at[b, :, cols]
            at = (kind, unit, part)
            away = remote(
                final.at[rows_of(1 - core, size), :], dst, osend.at[at], orecv.at[at], partner
            )
            away.start()
            stay = pltpu.make_async_copy(final.at[rows_of(core, size), :], dst, olocal.at[at])
            stay.start()
            outgoing.extend((away, stay))

    half = group * rrows
    lanes = 2 * half
    prompt_blocks = kp.shape[2] // block
    resp_blocks = kr.shape[3] // block
    base = chip * 2 * rrows
    factor = SCALE * LOG2E
    lane = lax.broadcasted_iota(jnp.int32, (1, lanes), 1)
    row_of = lax.rem(lane, rrows)
    positions = base + row_of + rrows * jnp.where(lane < half, core, 1 - core)
    key_iota = lax.broadcasted_iota(jnp.int32, (block, 1), 0)
    row_iota = lax.broadcasted_iota(jnp.int32, (rrows, 1), 0)
    nt = (((1,), (1,)), ((), ()))

    def key_rows(j):
        return pl.ds(pl.multiple_of(j * block, block), block)

    def compute(unit, ticks):
        k, b = units[unit]
        length = lengths[b]
        for source in range(2):
            owner = core if source == 0 else 1 - core
            live = base + owner * rrows + row_iota < length
            for g in range(group):
                cols = pl.ds((k * group + g) * HEAD_DIM, HEAD_DIM)
                at = pl.ds(source * half + g * rrows, rrows)
                qs[at, :] = qh[source, b, :, cols]
                rows = uh[source, b, :, cols]
                us[at, :] = jnp.where(live, rows, jnp.zeros_like(rows))
        m_buf[...] = jnp.full_like(m_buf, -jnp.inf)
        l_buf[...] = jnp.zeros_like(l_buf)
        e_buf[...] = jnp.zeros_like(e_buf)
        qt_buf[...] = jnp.zeros_like(qt_buf)
        ticks(0)

        def scores(keys, at, j, causal):
            s = lax.dot_general(keys, qs[...], nt, preferred_element_type=jnp.float32)
            if causal:
                s = jnp.where(key_iota + j * block <= positions, s, -jnp.inf)
            s_buf[at, :] = s
            m_buf[...] = jnp.maximum(m_buf[...], jnp.max(s, axis=0, keepdims=True))

        @pl.loop(0, prompt_blocks, unroll=True)
        def _(j):
            scores(kp[0, k, key_rows(j), :], key_rows(j), j, False)

        ticks(1)

        @pl.loop(0, resp_blocks, unroll=True)
        def _(j):
            scores(kr[0, k, b, key_rows(j), :], key_rows(prompt_blocks + j), j, True)

        ticks(2)
        shift = m_buf[...] * factor

        def weights(vals, at):
            p = jnp.exp2(s_buf[at, :] * factor - shift)
            d = lax.dot_general(vals, us[...], nt, preferred_element_type=jnp.float32)
            l_buf[...] += jnp.sum(p, axis=0, keepdims=True)
            e_buf[...] += jnp.sum(p * d, axis=0, keepdims=True)
            s_buf[at, :] = p
            d_buf[at, :] = d

        @pl.loop(0, prompt_blocks, unroll=True)
        def _(j):
            weights(kp[1, k, key_rows(j), :], key_rows(j))

        ticks(3)

        @pl.loop(0, resp_blocks, unroll=True)
        def _(j):
            weights(kr[1, k, b, key_rows(j), :], key_rows(prompt_blocks + j))

        ticks(4)
        inverse = 1.0 / l_buf[...]
        delta = e_buf[...] * inverse

        def grads(keys, at):
            p = s_buf[at, :] * inverse
            ds = (p * (d_buf[at, :] - delta)).astype(jnp.bfloat16)
            dv = jnp.dot(p.astype(jnp.bfloat16), us[...], preferred_element_type=jnp.float32)
            dk = jnp.dot(ds, qs[...], preferred_element_type=jnp.float32) * SCALE
            qt_buf[...] += jnp.dot(keys.T, ds, preferred_element_type=jnp.float32)
            return dk, dv

        @pl.loop(0, prompt_blocks, unroll=True)
        def _(j):
            at = key_rows(j)
            pair = grads(kp[0, k, at, :], at)
            for kind in range(2):
                if b == 0:
                    tp[kind, k, at, :] = pair[kind]
                else:
                    tp[kind, k, at, :] += pair[kind]

        ticks(5)

        @pl.loop(0, resp_blocks, unroll=True)
        def _(j):
            at = key_rows(j)
            pair = grads(kr[0, k, b, at, :], key_rows(prompt_blocks + j))
            for kind in range(2):
                tr[kind, k, b, at, :] = pair[kind]

        ticks(6)
        result = qt_buf[...].T * SCALE
        for source in range(2):
            for g in range(group):
                start = source * half + g * rrows
                dq[source, b, :, pl.ds((k * group + g) * HEAD_DIM, HEAD_DIM)] = result[
                    start : start + rrows
                ]
        span = group * HEAD_DIM
        cols = pl.ds(k * span, span)
        to = pl.ds(pl.multiple_of(core * wide + k * span, span), span)
        i = 2 + unit
        away = remote(dq.at[1, b, :, cols], gq.at[b, :, to], qsend.at[i], qrecv.at[i], partner)
        away.start()
        stay = pltpu.make_async_copy(dq.at[0, b, :, cols], gq.at[b, :, to], qlocal.at[i])
        stay.start()
        outgoing.extend((away, stay))

    last = len(units) - 1
    far = n // 2
    pulls = [(w - t + 1, t) for w in range(last + far) for t in range(1, far + 1) if 0 <= w - t + 1 <= last]
    pulls.sort(key=lambda hop: (2 * hop[0] + hop[1], hop[1]))

    def advance(count):
        for _ in range(min(count, len(pulls))):
            pull(*pulls.pop(0))

    first = pulls.index((0, far)) + 1
    advance(1)
    for copy in query_moves:
        copy.wait()
    advance(first - 1)
    pulled(0)
    per_tick = -(-len(pulls) // 12)
    due = {}
    for unit in range(last):
        for t in range(1, far + 1):
            when = (unit + 1) * TICKS + (t - 1) * 12 // far
            due.setdefault(min(when, (last + 1) * TICKS), []).append((unit, t))

    def push_all(unit, t):
        for part in reversed(parts_out(unit)):
            push(unit, t, part)
        if t == far:
            closing.append(unit)

    closing = []
    for unit in range(last + 1):

        def ticks(at, unit=unit):
            for which, t in due.get(unit * TICKS + at, []):
                push_all(which, t)
            if at > 0:
                advance(per_tick)
            if at == 5 and unit == last:
                push(unit, 1, 0)

        compute(unit, ticks)
        if unit < last:
            while any(hop[0] <= unit + 1 for hop in pulls):
                advance(1)
            pulled(unit + 1)
    push(last, 1, 1)
    for which, t in due.get((last + 1) * TICKS, []):
        push_all(which, t)
    for t in range(2, far + 1):
        push(last, t, 0)
        push(last, t, 1)
        if closing:
            which = closing.pop(0)
            for part in parts_out(which):
                finish(which, part)
    for which in closing:
        for part in parts_out(which):
            finish(which, part)
    finish(last, 0)
    finish(last, 1)
    for copy in moved.values():
        copy.wait_send()
    for copy in sent.values():
        copy.wait_send()
    for _, away, _ in entries:
        away.wait_send()
    for copy in outgoing:
        copy.wait()


def key_block(prompt, resp):
    size = 256
    while prompt % size or resp % size:
        size //= 2
    return size


def settle_kernel(*refs):
    count = (len(refs) - 2) // 3
    sources, targets, holds = refs[:count], refs[count : 2 * count], refs[2 * count : 3 * count]
    taken, given = refs[3 * count :]
    pieces = []
    for i, (source, target, hold) in enumerate(zip(sources, targets, holds)):
        chunks = 4 if source.size > 1 << 18 else 1
        step = source.shape[-1] // chunks
        for c in range(chunks):
            cut = (slice(None),) * (len(source.shape) - 1) + (pl.ds(c * step, step),)
            taking = pltpu.make_async_copy(source.at[cut], hold.at[cut], taken.at[i, c])
            taking.start()
            giving = pltpu.make_async_copy(hold.at[cut], target.at[cut], given.at[i, c])
            pieces.append((taking, giving))
    for taking, giving in pieces:
        taking.wait()
        giving.start()
    for _, giving in pieces:
        giving.wait()


def settle(*arrays):
    hbm = pl.BlockSpec(memory_space=pl.ANY)
    dma = pltpu.SemaphoreType.DMA
    return pl.pallas_call(
        settle_kernel,
        out_shape=tuple(jax.ShapeDtypeStruct(x.shape, x.dtype) for x in arrays),
        in_specs=[hbm] * len(arrays),
        out_specs=(hbm,) * len(arrays),
        scratch_shapes=[pltpu.VMEM(x.shape, x.dtype) for x in arrays]
        + [dma((len(arrays), 4)), dma((len(arrays), 4))],
        compiler_params=pltpu.CompilerParams(vmem_limit_bytes=60 * MIB),
        name="settle",
    )(*arrays)


def local(prompt_keys, prompt_values, queries, resp_keys, resp_values, cotangent, lengths):
    devices = lax.axis_size("ctx")
    n = devices // 2
    prows, columns = prompt_keys.shape
    rows, wide = queries.shape[1], queries.shape[2] // 2
    heads = columns // 2 // HEAD_DIM
    prompt, resp = prows * devices, rows * devices
    smem = pl.BlockSpec(memory_space=pltpu.SMEM)
    hbm = pl.BlockSpec(memory_space=pl.ANY)
    shape = jax.ShapeDtypeStruct
    bf16, f32 = jnp.bfloat16, jnp.float32
    vmem, dma = pltpu.VMEM, pltpu.SemaphoreType.DMA
    hop, units = n // 2, 2 * heads
    block = key_block(prompt, resp)
    lanes = 2 * rows * (wide // HEAD_DIM) // heads
    total = prompt + resp
    gq, grk, grv, gpk, gpv = pl.pallas_call(
        functools.partial(fused_kernel, n, block),
        out_shape=(
            shape((2, rows, 2 * wide), f32),
            shape((2, rows, columns), f32), shape((2, rows, columns), f32),
            shape((prows, columns), f32), shape((prows, columns), f32),
        ),
        in_specs=[smem] + [hbm] * 6,
        out_specs=(hbm,) * 5,
        scratch_shapes=[
            vmem((2, heads, prompt, HEAD_DIM), bf16),
            vmem((2, heads, 2, resp, HEAD_DIM), bf16),
            vmem((2, 2, rows, wide), bf16), vmem((2, 2, rows, wide), bf16),
            vmem((lanes, HEAD_DIM), bf16), vmem((lanes, HEAD_DIM), bf16),
            vmem((total, lanes), f32), vmem((total, lanes), f32),
            vmem((HEAD_DIM, lanes), f32),
            vmem((1, lanes), f32), vmem((1, lanes), f32), vmem((1, lanes), f32),
            vmem((2, heads, prompt, HEAD_DIM), f32),
            vmem((2, heads, 2, resp, HEAD_DIM), f32),
            vmem((2, 2, heads, hop, 2 * prows, HEAD_DIM), bf16),
            vmem((2, 2, units, hop, 2 * rows, HEAD_DIM), bf16),
            vmem((2, 2, heads, hop, 2 * prows, HEAD_DIM), bf16),
            vmem((2, 2, units, hop, 2 * rows, HEAD_DIM), bf16),
            vmem((2, heads, 2 * prows, HEAD_DIM), f32),
            vmem((2, heads, 2, 2 * rows, HEAD_DIM), f32),
            vmem((2, 2, rows, wide), f32),
            dma((2, 2, units, 2, hop)), dma((2, 2, units, 2, hop)),
            dma((2, 2, units, 2, hop)), dma((2, 2, units, 2, hop)),
            dma((2, units, 2)), dma((2, units, 2)), dma((2, units, 2)),
            dma((2 + units,)), dma((2 + units,)), dma((2 + units,)),
            dma((2, units, 2)), dma((2, units, 2)), dma((2, units, 2)),
        ],
        compiler_params=pltpu.CompilerParams(
            collective_id=0, has_side_effects=True, vmem_limit_bytes=60 * MIB
        ),
        name="fused",
    )(lengths, prompt_keys, prompt_values, resp_keys, resp_values, queries, cotangent)
    return settle(gq, grk, grv, gpk, gpv)


def solution(mesh):
    placed = (
        P(("pairs", "ctx"), None),
        P(("pairs", "ctx"), None),
        P("pairs", "ctx", None),
        P("pairs", "ctx", None),
        P("pairs", "ctx", None),
        P("pairs", "ctx", None),
        P("pairs"),
    )
    return jax.shard_map(
        local,
        mesh=mesh,
        in_specs=placed,
        out_specs=(
            P("pairs", "ctx", None),
            P("pairs", "ctx", None),
            P("pairs", "ctx", None),
            P(("pairs", "ctx"), None),
            P(("pairs", "ctx"), None),
        ),
        check_vma=False,
    )
```
